64 devices in a mesh: rep: 8 (over x, y, core), dp: 8 (over z).
Axes of the slice: x: 2, y: 2, z: 8, core: 2. Of those that a mesh axis runs over, the one named last changes fastest.
The devices are a block of a 4x4x8 slice.
Arguments:
- x: bfloat16 [64, 2048, 512], P(('rep', 'dp')), parts along dimension 0
- dy: bfloat16 [64, 2048, 512], P(('rep', 'dp')), parts along dimension 0
- wq: bfloat16 [2, 512, 512], replicated
- wk: bfloat16 [2, 512, 512], replicated
- wv: bfloat16 [2, 512, 512], replicated
- wo: bfloat16 [2, 512, 512], replicated
- w_gate: bfloat16 [2, 512, 2048], replicated
- w_up: bfloat16 [2, 512, 2048], replicated
- w_down: bfloat16 [2, 2048, 512], replicated
- m_wq: float32 [2, 512, 512], P(None, 'dp')
- m_wk: float32 [2, 512, 512], P(None, 'dp')
- m_wv: float32 [2, 512, 512], P(None, 'dp')
- m_wo: float32 [2, 512, 512], P(None, 'dp')
- m_w_gate: float32 [2, 512, 2048], P(None, 'dp')
- m_w_up: float32 [2, 512, 2048], P(None, 'dp')
- m_w_down: float32 [2, 2048, 512], P(None, 'dp')
- v_wq: float32 [2, 512, 512], P(None, 'dp')
- v_wk: float32 [2, 512, 512], P(None, 'dp')
- v_wv: float32 [2, 512, 512], P(None, 'dp')
- v_wo: float32 [2, 512, 512], P(None, 'dp')
- v_w_gate: float32 [2, 512, 2048], P(None, 'dp')
- v_w_up: float32 [2, 512, 2048], P(None, 'dp')
- v_w_down: float32 [2, 2048, 512], P(None, 'dp')
Outputs:
- output 1: bfloat16 [16, 512, 512], P('rep'), parts along dimension 0
- output 2: bfloat16 [16, 512, 512], P('rep'), parts along dimension 0
- output 3: bfloat16 [16, 512, 512], P('rep'), parts along dimension 0
- output 4: bfloat16 [16, 512, 512], P('rep'), parts along dimension 0
- output 5: bfloat16 [16, 512, 2048], P('rep'), parts along dimension 0
- output 6: bfloat16 [16, 512, 2048], P('rep'), parts along dimension 0
- output 7: bfloat16 [16, 2048, 512], P('rep'), parts along dimension 0
- output 8: float32 [16, 512, 512], P('rep', 'dp'), parts along dimension 0
- output 9: float32 [16, 512, 512], P('rep', 'dp'), parts along dimension 0
- output 10: float32 [16, 512, 512], P('rep', 'dp'), parts along dimension 0
- output 11: float32 [16, 512, 512], P('rep', 'dp'), parts along dimension 0
- output 12: float32 [16, 512, 2048], P('rep', 'dp'), parts along dimension 0
- output 13: float32 [16, 512, 2048], P('rep', 'dp'), parts along dimension 0
- output 14: float32 [16, 2048, 512], P('rep', 'dp'), parts along dimension 0
- output 15: float32 [16, 512, 512], P('rep', 'dp'), parts along dimension 0
- output 16: float32 [16, 512, 512], P('rep', 'dp'), parts along dimension 0
- output 17: float32 [16, 512, 512], P('rep', 'dp'), parts along dimension 0
- output 18: float32 [16, 512, 512], P('rep', 'dp'), parts along dimension 0
- output 19: float32 [16, 512, 2048], P('rep', 'dp'), parts along dimension 0
- output 20: float32 [16, 512, 2048], P('rep', 'dp'), parts along dimension 0
- output 21: float32 [16, 2048, 512], P('rep', 'dp'), parts along dimension 0
There are 8 independent parts. The reference program is written for one: setup_inputs(seed, part) draws one part's arguments, and reference() takes and returns one part's arrays. A program takes and returns all parts, laid end to end along the dimension named above; an argument that names none is the same for every part.
All inputs are finite; a program needn't handle non-finite values.
Results may differ from the reference program's by a relative error of at most 0.024.
Values are sent between devices in bfloat16 or wider.
A program may use at most 768 MiB of HBM per device.

```python
import jax
import jax.numpy as jnp
from jax import lax

SEQUENCES = 8
TOKENS = 2048
D = 512
HEADS = 2
KV_HEADS = 2
HEAD = 256
FF = 2048
LAYERS = 2
THETA = 10000
NAMES = ("wq", "wk", "wv", "wo", "w_gate", "w_up", "w_down")
SHAPES = {
    "wq": (LAYERS, D, HEADS * HEAD),
    "wk": (LAYERS, D, KV_HEADS * HEAD),
    "wv": (LAYERS, D, KV_HEADS * HEAD),
    "wo": (LAYERS, HEADS * HEAD, D),
    "w_gate": (LAYERS, D, FF),
    "w_up": (LAYERS, D, FF),
    "w_down": (LAYERS, FF, D),
}


def bump(key, n, height):
    away = (jnp.arange(n, dtype=jnp.int32) - jax.random.randint(key, (), 0, n, jnp.int32)) % n
    return jnp.where(away < n // 8, height, 1.0)


def together(key, own, strength):
    shared = jax.random.normal(key, own.shape[1:], jnp.float32)
    return (own + strength * shared) * lax.rsqrt(1 + strength * strength)


def setup_inputs(seed: int = 0, part: int = 0) -> dict:
    kx, kdy, ka, kb, kz, kf, kh, kl, *keys = jax.random.split(jax.random.key(seed), 8 + 3 * len(NAMES))
    kx, kdy, ka, kb = (jax.random.fold_in(k, part) for k in (kx, kdy, ka, kb))
    kw, km, kv = (keys[i::3] for i in range(3))
    shape = (SEQUENCES, TOKENS, D)
    much_x, much_dy = jax.random.uniform(kz, (2,), jnp.float32, 0.0, 1.0)
    loud = 2.0 ** jax.random.uniform(jax.random.fold_in(kz, 1), (), jnp.float32, -1.0, 2.0)
    layers = 2.0 ** jax.random.uniform(kl, (LAYERS, 1, 1), jnp.float32, -1.0, 1.0)
    times = {"wq": 1.0, "wk": 1.0, "wv": 2.0, "wo": layers, "w_gate": 1.0, "w_up": bump(kh, FF, 4.0), "w_down": layers}
    x = together(ka, jax.random.normal(kx, shape, jnp.float32), much_x) * bump(kf, D, 4.0)
    dy = together(kb, jax.random.normal(kdy, shape, jnp.float32), much_dy)
    drawn = {"x": x.astype(jnp.bfloat16), "dy": (loud * dy * (SEQUENCES * TOKENS) ** -0.5).astype(jnp.bfloat16)}
    for key, name in zip(kw, NAMES, strict=True):
        drawn[name] = (jax.random.normal(key, SHAPES[name], jnp.float32) * SHAPES[name][1] ** -0.5 * times[name]).astype(jnp.bfloat16)
    for key, name in zip(km, NAMES, strict=True):
        drawn[f"m_{name}"] = 0.1 * jax.random.normal(key, SHAPES[name], jnp.float32)
    for key, name in zip(kv, NAMES, strict=True):
        drawn[f"v_{name}"] = jax.random.uniform(key, SHAPES[name], jnp.float32, 0.02, 0.06)
    return drawn


def matmul(a, w):
    return jnp.dot(a, w, preferred_element_type=jnp.float32).astype(jnp.bfloat16)


def normed(h):
    wide = h.astype(jnp.float32)
    scale = lax.rsqrt(jnp.mean(wide**2, -1, keepdims=True) + 1e-6)
    return (wide * scale).astype(jnp.bfloat16)


def turned(t, theta):
    half = t.shape[-1] // 2
    angle = jnp.arange(t.shape[0], dtype=jnp.float32)[:, None] * theta ** (-jnp.arange(half, dtype=jnp.float32) / half)
    cos, sin = jnp.cos(angle)[:, None], jnp.sin(angle)[:, None]
    a, b = t[..., :half].astype(jnp.float32), t[..., half:].astype(jnp.float32)
    return jnp.concatenate([a * cos - b * sin, b * cos + a * sin], -1).astype(jnp.bfloat16)


def seen_by(q, k, v):
    tokens, kv = q.shape[0], k.shape[1]
    q = q.reshape(tokens, kv, -1, q.shape[-1])
    scores = jnp.einsum("tgsd,ugd->gstu", q.astype(jnp.float32), k.astype(jnp.float32)) * q.shape[-1] ** -0.5
    place = jnp.arange(tokens)
    weights = jax.nn.softmax(jnp.where(place[:, None] >= place, scores, -jnp.inf), -1).astype(jnp.bfloat16)
    return jnp.einsum("gstu,ugd->tgsd", weights.astype(jnp.float32), v.astype(jnp.float32)).astype(jnp.bfloat16).reshape(tokens, -1)


def layer(h, w):
    a = normed(h)
    q, k = (turned(matmul(a, w[name]).reshape(h.shape[0], -1, HEAD), THETA) for name in ("wq", "wk"))
    h = h + matmul(seen_by(q, k, matmul(a, w["wv"]).reshape(h.shape[0], -1, HEAD)), w["wo"])
    b = normed(h)
    gate = jnp.dot(b, w["w_gate"], preferred_element_type=jnp.float32)
    up = jnp.dot(b, w["w_up"], preferred_element_type=jnp.float32)
    return h + matmul((jax.nn.silu(gate) * up).astype(jnp.bfloat16), w["w_down"])


def adamw(w, m, v, g):
    m = 0.9 * m + 0.1 * g
    v = 0.95 * v + 0.05 * g * g
    step = m * lax.rsqrt(v + 1e-8) + 0.1 * w
    return (w - 0.02 * step).astype(jnp.bfloat16), m, v


def clipped(gradients, sum_of_squares, count):
    factor = jnp.minimum(1.0, 0.5 * lax.rsqrt(sum_of_squares / count + 1e-30))
    return [g * factor for g in gradients]


def stack(weights, h):
    return lax.scan(lambda h, w: (layer(h, w), None), h, weights)[0]


def reference(x, dy, wq, wk, wv, wo, w_gate, w_up, w_down, m_wq, m_wk, m_wv, m_wo, m_w_gate, m_w_up, m_w_down, v_wq, v_wk, v_wv, v_wo, v_w_gate, v_w_up, v_w_down):
    weights = dict(zip(NAMES, (wq, wk, wv, wo, w_gate, w_up, w_down), strict=True))

    def take(so_far, sequence):
        h, by_y = sequence
        _, back = jax.vjp(stack, weights, h)
        by_weights, by_h = back(by_y)
        return jax.tree.map(lambda total, term: total + term.astype(jnp.float32), so_far, by_weights), by_h

    none_yet = {name: jnp.zeros(w.shape, jnp.float32) for name, w in weights.items()}
    by_weights, by_x = lax.scan(take, none_yet, (x, dy))
    gradients = [by_weights[name].astype(jnp.bfloat16).astype(jnp.float32) for name in NAMES]
    gradients = clipped(gradients, sum(jnp.sum(g * g) for g in gradients), sum(g.size for g in gradients))
    first = (m_wq, m_wk, m_wv, m_wo, m_w_gate, m_w_up, m_w_down)
    second = (v_wq, v_wk, v_wv, v_wo, v_w_gate, v_w_up, v_w_down)
    new = [adamw(weights[name].astype(jnp.float32), m, v, g) for name, m, v, g in zip(NAMES, first, second, gradients, strict=True)]
    return tuple(one[which] for which in range(3) for one in new)
```

```python
import functools

import jax
import jax.numpy as jnp
from jax import lax
from jax.experimental import pallas as pl
from jax.experimental.pallas import tpu as pltpu
from jax.sharding import PartitionSpec as P

HEAD = 256
THETA = 10000
NAMES = ("wq", "wk", "wv", "wo", "w_gate", "w_up", "w_down")
FFN = ("w_gate", "w_up", "w_down", "wo")
QKV = ("wq", "wk", "wv")
NEG = -1e30
HIDDEN = 2 * NEG
LOG2E = 1.4426950408889634
VMEM = 60 * 2**20
F32, BF = jnp.float32, jnp.bfloat16
BLOCK = 512


def _dot(a, b, ca, cb):
    return lax.dot_general(a, b, (((ca,), (cb,)), ((), ())), preferred_element_type=F32)


def _params(n):
    return pltpu.CompilerParams(dimension_semantics=("arbitrary",) * n, vmem_limit_bytes=VMEM)


def _cost(flops, *arrays, exps=0):
    return pl.CostEstimate(flops=int(flops), transcendentals=int(exps), bytes_accessed=int(sum(a.size * a.dtype.itemsize for a in arrays)))


def _norm(h):
    wide = h.astype(F32)
    scale = lax.rsqrt(jnp.mean(wide * wide, -1, keepdims=True) + 1e-6)
    return (wide * scale).astype(BF), wide, scale


def _norm_bwd(wide, scale, d):
    inner = jnp.mean(d * wide, -1, keepdims=True)
    return scale * d - wide * (scale * scale * scale * inner)


def _rows(block, width):
    return pl.BlockSpec((block, width), lambda i: (i, 0))


def _layer_of(w, number):
    return pl.BlockSpec((1, *w.shape[1:]), lambda *_: (number, 0, 0), pipeline_mode=pl.Buffered(1))


def _whole(shape):
    return pl.BlockSpec(shape, lambda *_: (0,) * len(shape))


def _halves(cols):
    half = HEAD // 2
    return [(slice(at, at + half), slice(at + half, at + HEAD)) for at in range(0, cols, HEAD)]


def _qkv(h_ref, cos_ref, sin_ref, wq_ref, wk_ref, wv_ref, q_ref, k_ref, v_ref):
    a, _, _ = _norm(h_ref[...])
    cos, sin = cos_ref[...], sin_ref[...]
    for w_ref, o_ref in ((wq_ref, q_ref), (wk_ref, k_ref)):
        t = _dot(a, w_ref[0], 1, 0).astype(BF).astype(F32)
        for one, two in _halves(t.shape[1]):
            o_ref[:, one] = (t[:, one] * cos - t[:, two] * sin).astype(BF)
            o_ref[:, two] = (t[:, two] * cos + t[:, one] * sin).astype(BF)
    v_ref[...] = _dot(a, wv_ref[0], 1, 0).astype(BF)


def qkv(h, cos, sin, w, number):
    t, d = h.shape
    bt = min(BLOCK, t)
    ws = [w[n] for n in QKV]
    outs = [jax.ShapeDtypeStruct((t, x.shape[2]), BF) for x in ws]
    return pl.pallas_call(
        _qkv,
        grid=(t // bt,),
        in_specs=[_rows(bt, d), _rows(bt, HEAD // 2), _rows(bt, HEAD // 2)] + [_layer_of(x, number) for x in ws],
        out_specs=[_rows(bt, x.shape[1]) for x in outs],
        out_shape=outs,
        compiler_params=_params(1),
        cost_estimate=_cost(2 * t * d * sum(x.shape[2] for x in ws), h, *outs),
        name="qkv",
    )(h, cos, sin, *ws)


def _triangle(n):
    return lax.broadcasted_iota(jnp.int32, (n, n), 1) >= lax.broadcasted_iota(jnp.int32, (n, n), 0)


def _forward(q_ref, k_ref, v_ref, o_ref, lse_ref, top_s, mix_s, *, bq):
    i = pl.program_id(0)
    heads = [(n, slice(n * HEAD, (n + 1) * HEAD)) for n in range(q_ref.shape[1] // HEAD)]
    scale = HEAD**-0.5
    e = scale * LOG2E
    top_s[...] = jnp.full(top_s.shape, NEG, F32)
    mix_s[...] = jnp.zeros_like(mix_s)
    ones = jnp.ones((8, bq), BF)

    def block(j, masked):
        here = pl.ds(pl.multiple_of(j * bq, bq), bq)
        scores = [_dot(k_ref[here, at], q_ref[:, at], 1, 1) for _, at in heads]
        weights, keeps = [], []
        for (n, at), s in zip(heads, scores):
            if masked:
                s = jnp.where(_triangle(bq), s, HIDDEN)
            old = top_s[n : n + 1, :]
            top = jnp.maximum(old, s.max(axis=0, keepdims=True))
            top_s[n : n + 1, :] = top
            weights.append(jnp.exp2((s - top) * e).astype(BF))
            keeps.append(jnp.exp2((old - top) * e))
        for (n, at), p, keep in zip(heads, weights, keeps):
            values = jnp.concatenate([v_ref[here, at].T, ones], axis=0)
            mix_s[n] = mix_s[n] * keep + _dot(values, p, 1, 0)

    lax.fori_loop(0, i, lambda j, _: block(j, False), None)
    block(i, True)
    for n, at in heads:
        total = mix_s[n, HEAD : HEAD + 1, :]
        o_ref[:, at] = (mix_s[n, :HEAD, :] * (1 / total)).T.astype(BF)
        lse_ref[n : n + 1, :] = top_s[n : n + 1, :] * scale + jnp.log(total)


def attend(q, k, v):
    t, cols = q.shape
    bq, n = min(BLOCK, t), cols // HEAD
    return pl.pallas_call(
        functools.partial(_forward, bq=bq),
        grid=(t // bq,),
        in_specs=[_rows(bq, cols), _whole(k.shape), _whole(v.shape)],
        out_specs=[_rows(bq, cols), pl.BlockSpec((n, bq), lambda i: (0, i))],
        out_shape=[jax.ShapeDtypeStruct((t, cols), BF), jax.ShapeDtypeStruct((n, t), F32)],
        scratch_shapes=[pltpu.VMEM((n, bq), F32), pltpu.VMEM((n, HEAD + 8, bq), F32)],
        compiler_params=_params(1),
        cost_estimate=_cost(4 * t * t * cols, q, k, v, q, exps=t * t * n),
        name="attend",
    )(q, k, v)


def _backward(q_ref, k_ref, v_ref, o_ref, do_ref, lse_ref, dq_ref, dk_ref, dv_ref, dq_s, dk_s, dv_s, *, bq):
    i = pl.program_id(0)
    heads = [(n, slice(n * HEAD, (n + 1) * HEAD)) for n in range(q_ref.shape[1] // HEAD)]
    scale = HEAD**-0.5
    e = scale * LOG2E

    @pl.when(i == 0)
    def _():
        dk_s[...] = jnp.zeros_like(dk_s)
        dv_s[...] = jnp.zeros_like(dv_s)

    dq_s[...] = jnp.zeros_like(dq_s)
    lses = [lse_ref[n : n + 1, :] * LOG2E for n, _ in heads]
    deltas = []
    for _, at in heads:
        both = do_ref[:, at].astype(F32) * o_ref[:, at].astype(F32)
        deltas.append((both[:, : HEAD // 2] + both[:, HEAD // 2 :]).T.sum(axis=0, keepdims=True))

    def block(j, masked):
        here = pl.ds(pl.multiple_of(j * bq, bq), bq)
        scores = [_dot(k_ref[here, at], q_ref[:, at], 1, 1) for _, at in heads]
        dps = [_dot(v_ref[here, at], do_ref[:, at], 1, 1) for _, at in heads]
        for n, at in heads:
            p = jnp.exp2(scores[n] * e - lses[n])
            if masked:
                p = jnp.where(_triangle(bq), p, 0.0)
            ds = (p * (dps[n] - deltas[n])).astype(BF)
            dv_s[here, at] += _dot(p.astype(BF), do_ref[:, at], 1, 0)
            dk_s[here, at] += _dot(ds, q_ref[:, at], 1, 0)
            dq_s[n] += _dot(k_ref[here, at].T, ds, 1, 0)

    lax.fori_loop(0, i, lambda j, _: block(j, False), None)
    block(i, True)
    for n, at in heads:
        dq_ref[:, at] = (dq_s[n] * scale).T.astype(BF)

    @pl.when(i == pl.num_programs(0) - 1)
    def _():
        dk_ref[...] = (dk_s[...] * scale).astype(BF)
        dv_ref[...] = dv_s[...].astype(BF)


def attend_bwd(q, k, v, o, do, lse):
    t, cols = q.shape
    bq, n = min(BLOCK, t), cols // HEAD
    out = jax.ShapeDtypeStruct((t, cols), BF)
    return pl.pallas_call(
        functools.partial(_backward, bq=bq),
        grid=(t // bq,),
        in_specs=[_rows(bq, cols), _whole(k.shape), _whole(v.shape), _rows(bq, cols), _rows(bq, cols), pl.BlockSpec((n, bq), lambda i: (0, i))],
        out_specs=[_rows(bq, cols), _whole(k.shape), _whole(v.shape)],
        out_shape=[out] * 3,
        scratch_shapes=[pltpu.VMEM((n, HEAD, bq), F32), pltpu.VMEM((t, cols), F32), pltpu.VMEM((t, cols), F32)],
        compiler_params=_params(1),
        cost_estimate=_cost(6 * t * t * cols, q, k, v, o, do, out, out, out, exps=t * t * n),
        name="attend_bwd",
    )(q, k, v, o, do, lse)


def _ffn(h_ref, o_ref, wo_ref, wg_ref, wu_ref, wd_ref, out_ref, *, piece):
    h2 = h_ref[...] + _dot(o_ref[...], wo_ref[0], 1, 0).astype(BF)
    b, _, _ = _norm(h2)
    total = 0.0
    for at in range(0, wd_ref.shape[1], piece):
        cut = slice(at, at + piece)
        gate, up = _dot(b, wg_ref[0, :, cut], 1, 0), _dot(b, wu_ref[0, :, cut], 1, 0)
        act = (gate * (1 / (1 + jnp.exp(-gate))) * up).astype(BF)
        total = total + _dot(act, wd_ref[0, cut, :], 1, 0)
    out_ref[...] = h2 + total.astype(BF)


def ffn(h, o, w, number):
    t, d = h.shape
    bt = min(BLOCK, t)
    ws = [w[n] for n in ("wo", "w_gate", "w_up", "w_down")]
    ff = w["w_down"].shape[1]
    return pl.pallas_call(
        functools.partial(_ffn, piece=min(512, ff)),
        grid=(t // bt,),
        in_specs=[_rows(bt, d), _rows(bt, o.shape[1])] + [_layer_of(x, number) for x in ws],
        out_specs=_rows(bt, d),
        out_shape=jax.ShapeDtypeStruct((t, d), BF),
        compiler_params=_params(1),
        cost_estimate=_cost(2 * t * d * (o.shape[1] + 3 * ff), h, o, h, exps=t * ff),
        name="ffn",
    )(h, o, *ws)


def _pack(out_ref, at, acc, panels):
    n, width = out_ref.shape[0], out_ref.shape[2]
    rows = acc.shape[0] // n
    for j in range(n):
        for p in range(panels):
            out_ref[j, at + p * rows : at + (p + 1) * rows, :] = acc[j * rows : (j + 1) * rows, p * width : (p + 1) * width].astype(BF)
    return at + panels * rows


def _ffn_bwd(h_ref, o_ref, dy_ref, wo_ref, wg_ref, wu_ref, wd_ref, do_ref, dh_ref, out_ref, g_s, u_s, d_s, o_s, *, piece):
    i = pl.program_id(0)

    @pl.when(i == 0)
    def _():
        for s in (g_s, u_s, d_s, o_s):
            s[...] = jnp.zeros_like(s)

    o, dy = o_ref[...], dy_ref[...]
    h2 = h_ref[...] + _dot(o, wo_ref[0], 1, 0).astype(BF)
    b, wide, scale = _norm(h2)
    by_gate, by_up = 0.0, 0.0
    for at in range(0, wd_ref.shape[1], piece):
        cut = slice(at, at + piece)
        gate, up = _dot(b, wg_ref[0, :, cut], 1, 0), _dot(b, wu_ref[0, :, cut], 1, 0)
        d = _dot(dy, wd_ref[0, cut, :], 1, 1).astype(BF).astype(F32)
        sig = 1 / (1 + jnp.exp(-gate))
        silu = gate * sig
        act = (silu * up).astype(BF)
        d_up = (d * silu).astype(BF)
        d_gate = (d * up * (sig + silu * (1 - sig))).astype(BF)
        d_s[cut, :] += _dot(act, dy, 0, 0)
        g_s[:, cut] += _dot(b, d_gate, 0, 0)
        u_s[:, cut] += _dot(b, d_up, 0, 0)
        by_gate = by_gate + _dot(d_gate, wg_ref[0, :, cut], 1, 1)
        by_up = by_up + _dot(d_up, wu_ref[0, :, cut], 1, 1)
    by_b = (by_gate.astype(BF) + by_up.astype(BF)).astype(F32)
    dh = dy + _norm_bwd(wide, scale, by_b).astype(BF)
    dh_ref[...] = dh
    do_ref[...] = _dot(dh, wo_ref[0], 1, 1).astype(BF)
    o_s[...] += _dot(o, dh, 0, 0)

    @pl.when(i == pl.num_programs(0) - 1)
    def _():
        at = 0
        for s in (g_s, u_s, d_s, o_s):
            at = _pack(out_ref, at, s, s.shape[1] // out_ref.shape[2])


def ffn_bwd(h, o, dy, w, number, n):
    t, d = h.shape
    bt = min(BLOCK, t)
    ws = [w[x] for x in ("wo", "w_gate", "w_up", "w_down")]
    ff, cols = w["w_down"].shape[1], o.shape[1]
    rows = sum(w[x].shape[1] * w[x].shape[2] for x in FFN) // (n * d)
    packed = jax.ShapeDtypeStruct((n, sum(x[0].size for x in w.values()) // (n * d), d), BF)
    return pl.pallas_call(
        functools.partial(_ffn_bwd, piece=min(512, ff)),
        grid=(t // bt,),
        in_specs=[_rows(bt, d), _rows(bt, cols), _rows(bt, d)] + [_layer_of(x, number) for x in ws],
        out_specs=[_rows(bt, cols), _rows(bt, d), pl.BlockSpec((n, rows, d), lambda i: (0, 0, 0), pipeline_mode=pl.Buffered(1))],
        out_shape=[jax.ShapeDtypeStruct((t, cols), BF), jax.ShapeDtypeStruct((t, d), BF), packed],
        scratch_shapes=[pltpu.VMEM((d, ff), F32), pltpu.VMEM((d, ff), F32), pltpu.VMEM((ff, d), F32), pltpu.VMEM((cols, d), F32)],
        compiler_params=_params(1),
        cost_estimate=_cost(2 * t * d * (3 * cols + 8 * ff), h, o, dy, h, o, packed, exps=t * ff),
        name="ffn_bwd",
    )(h, o, dy, *ws)


def _qkv_bwd(h_ref, cos_ref, sin_ref, dq_ref, dk_ref, dv_ref, _, *rest, first, at):
    ins, rest = ([], rest) if first else (rest[:4], rest[4:])
    dh_ref, rest = (None, rest) if first else (rest[0], rest[1:])
    out_ref, pack_s, sem, *sums = rest
    i = pl.program_id(0)

    @pl.when(i == 0)
    def _():
        for s in sums:
            s[...] = jnp.zeros_like(s)

    a, wide, scale = _norm(h_ref[...])
    cos, sin = cos_ref[...], sin_ref[...]
    parts = []
    for d_ref in (dq_ref, dk_ref):
        t = d_ref[...].astype(F32)
        pieces = []
        for one, two in _halves(t.shape[1]):
            pieces += [(t[:, one] * cos + t[:, two] * sin).astype(BF), (t[:, two] * cos - t[:, one] * sin).astype(BF)]
        parts.append(jnp.concatenate(pieces, axis=1))
    parts.append(dv_ref[...])
    for s, p in zip(sums, parts):
        s[...] += _dot(a, p, 0, 0)
    if not first:
        dh2_ref, *ws = ins
        by_a = sum(_dot(p, w[0], 1, 1).astype(BF).astype(F32) for p, w in zip(parts, ws))
        dh_ref[...] = dh2_ref[...] + _norm_bwd(wide, scale, by_a).astype(BF)

    @pl.when(i == pl.num_programs(0) - 1)
    def _():
        to = 0
        for s in sums:
            to = _pack(pack_s, to, s, s.shape[1] // pack_s.shape[2])
        copy = pltpu.make_async_copy(pack_s, out_ref.at[:, at : at + to, :], sem)
        copy.start()
        copy.wait()


def qkv_bwd(h, cos, sin, grads, packed, dh, w, number, n):
    t, d = h.shape
    bt = min(BLOCK, t)
    ws = [w[x] for x in QKV]
    rows = sum(x.shape[1] * x.shape[2] for x in ws) // (n * d)
    first = dh is None
    more = [] if first else [dh, *ws]
    got = pl.pallas_call(
        functools.partial(_qkv_bwd, first=first, at=packed.shape[1] - rows),
        grid=(t // bt,),
        in_specs=[_rows(bt, d), _rows(bt, HEAD // 2), _rows(bt, HEAD // 2)] + [_rows(bt, g.shape[1]) for g in grads] + [pl.BlockSpec(memory_space=pl.ANY)]
        + ([] if first else [_rows(bt, d)] + [_layer_of(x, number) for x in ws]),
        out_specs=([] if first else [_rows(bt, d)]) + [pl.BlockSpec(memory_space=pl.ANY)],
        out_shape=([] if first else [jax.ShapeDtypeStruct((t, d), BF)]) + [jax.ShapeDtypeStruct(packed.shape, BF)],
        input_output_aliases={6: 0 if first else 1},
        scratch_shapes=[pltpu.VMEM((n, rows, d), BF), pltpu.SemaphoreType.DMA] + [pltpu.VMEM(x.shape[1:], F32) for x in ws],
        compiler_params=_params(1),
        cost_estimate=_cost(2 * t * d * (1 if first else 2) * sum(x.shape[2] for x in ws), h, *grads),
        name="qkv_bwd",
    )(h, cos, sin, *grads, packed, *more)
    return (None, got[0]) if first else got


def _adamw(me_ref, factor_ref, *refs, layers, count):
    g_refs, refs = refs[:layers], refs[layers:]
    w_refs, m_refs, v_refs, nm_refs, nv_refs = (dict(zip(NAMES, refs[i * count : (i + 1) * count])) for i in range(5))
    out_ref = refs[5 * count]
    factor = factor_ref[0]
    width = out_ref.shape[2]
    for number in range(layers):
        at = 0
        for name in FFN + QKV:
            rows, cols = w_refs[name].shape[1:]
            for p in range(cols // width):
                cut = slice(p * width, (p + 1) * width)
                g = g_refs[number][at : at + rows, :].astype(F32) * factor
                m = 0.9 * m_refs[name][number, :, cut] + 0.1 * g
                v = 0.95 * v_refs[name][number, :, cut] + 0.05 * g * g
                w = w_refs[name][number, :, cut].astype(F32)
                nm_refs[name][number, :, cut] = m
                nv_refs[name][number, :, cut] = v
                out_ref[number, at : at + rows, :] = (w - 0.02 * (m * lax.rsqrt(v + 1e-8) + 0.1 * w)).astype(BF)
                at += rows


def adamw(me, factor, shares, weights, m, v):
    layers, d = weights[0].shape[0], shares[0].shape[1]
    rows = sum(x.shape[0] for x in shares) // layers
    own = [pl.BlockSpec((layers, *one.shape[1:]), lambda i, me: (0, me[0], 0)) for one in m]
    here = [pl.BlockSpec(one.shape, lambda i, me: (0, 0, 0)) for one in m]
    got = pl.pallas_call(
        functools.partial(_adamw, layers=layers, count=len(m)),
        grid_spec=pltpu.PrefetchScalarGridSpec(
            num_scalar_prefetch=1,
            grid=(1,),
            in_specs=[pl.BlockSpec(memory_space=pltpu.SMEM)] + [pl.BlockSpec(x.shape, lambda i, me: (0, 0)) for x in shares] + own + here + here,
            out_specs=here + here + [pl.BlockSpec((layers, rows, d), lambda i, me: (0, 0, 0))],
        ),
        out_shape=[jax.ShapeDtypeStruct(x.shape, F32) for x in (*m, *m)] + [jax.ShapeDtypeStruct((layers, rows, d), BF)],
        compiler_params=_params(1),
        cost_estimate=_cost(20 * layers * rows * d, *m, *m, *m, *m),
        name="adamw",
    )(me[None], factor[None], *shares, *weights, *m, *v)
    k = len(m)
    return got[:k], got[k : 2 * k], got[2 * k]


def _unpack(in_ref, *out_refs):
    outs = dict(zip(NAMES, out_refs))
    width = in_ref.shape[3]
    for number in range(in_ref.shape[1]):
        at = 0
        for name in FFN + QKV:
            rows, cols = outs[name].shape[1:]
            for p in range(cols // width):
                outs[name][number, :, p * width : (p + 1) * width] = in_ref[0, number, at : at + rows, :]
                at += rows


def unpack(packed, shapes):
    n = packed.shape[0]
    return pl.pallas_call(
        _unpack,
        grid=(n,),
        in_specs=[pl.BlockSpec((1, *packed.shape[1:]), lambda j: (j, 0, 0, 0))],
        out_specs=[pl.BlockSpec((s[0], s[1] // n, s[2]), lambda j: (0, j, 0)) for s in shapes],
        out_shape=[jax.ShapeDtypeStruct(s, BF) for s in shapes],
        compiler_params=_params(1),
        cost_estimate=_cost(0, packed, packed),
        name="unpack",
    )(packed)


def solution(mesh):
    n = mesh.shape["dp"]

    def step(x, dy, *arrays):
        weights, m, v = (arrays[i : i + 7] for i in (0, 7, 14))
        w = dict(zip(NAMES, weights, strict=True))
        layers = weights[0].shape[0]
        half = HEAD // 2
        angle = jnp.arange(x.shape[1], dtype=F32)[:, None] * THETA ** (-jnp.arange(half, dtype=F32) / half)
        cos, sin = jnp.cos(angle), jnp.sin(angle)
        h, kept = x[0], []
        for number in range(layers):
            q, k, val = qkv(h, cos, sin, w, number)
            o, lse = attend(q, k, val)
            kept.append((h, q, k, val, o, lse))
            if number < layers - 1:
                h = ffn(h, o, w, number)
        d, shares = dy[0], [None] * layers
        scatter = lambda g: lax.psum_scatter(g, "dp", scatter_dimension=0, tiled=False)
        for number in reversed(range(layers)):
            h, q, k, val, o, lse = kept[number]
            do, dh, packed = ffn_bwd(h, o, d, w, number, n)
            grads = attend_bwd(q, k, val, o, do, lse)
            d, packed = qkv_bwd(h, cos, sin, grads, packed, dh if number else None, w, number, n)
            shares[number] = scatter(packed)
        squares = lax.psum(sum(jnp.sum(g.astype(F32) ** 2) for g in shares), "dp")
        count = n * sum(g.size for g in shares)
        factor = jnp.minimum(1.0, 0.5 * lax.rsqrt(squares / count + 1e-30))
        new_m, new_v, packed = adamw(lax.axis_index("dp"), factor, shares, weights, m, v)
        new_w = unpack(lax.all_gather(packed, "dp", axis=0, tiled=False), [one.shape for one in weights])
        return (*new_w, *new_m, *new_v)

    states, all_of, cut = P(("rep", "dp"), None, None), P(None, None, None), P(None, "dp", None)
    return jax.shard_map(
        step,
        mesh=mesh,
        in_specs=(states, states) + (all_of,) * 7 + (cut,) * 14,
        out_specs=(P("rep", None, None),) * 7 + (P("rep", "dp", None),) * 14,
        check_vma=False,
    )
```

```python
import functools

import jax
import jax.numpy as jnp
from jax import lax
from jax.experimental import pallas as pl
from jax.experimental.pallas import tpu as pltpu
from jax.sharding import PartitionSpec as P

HEAD = 256
THETA = 10000
NAMES = ("wq", "wk", "wv", "wo", "w_gate", "w_up", "w_down")
FFN = ("w_gate", "w_up", "w_down", "wo")
QKV = ("wq", "wk", "wv")
NEG = -1e30
HIDDEN = 2 * NEG
LOG2E = 1.4426950408889634
VMEM = 60 * 2**20
F32, BF = jnp.float32, jnp.bfloat16
BLOCK = 512


def _dot(a, b, ca, cb):
    return lax.dot_general(a, b, (((ca,), (cb,)), ((), ())), preferred_element_type=F32)


def _params(n):
    return pltpu.CompilerParams(dimension_semantics=("arbitrary",) * n, vmem_limit_bytes=VMEM)


def _cost(flops, *arrays, exps=0):
    return pl.CostEstimate(flops=int(flops), transcendentals=int(exps), bytes_accessed=int(sum(a.size * a.dtype.itemsize for a in arrays)))


def _norm(h):
    wide = h.astype(F32)
    scale = lax.rsqrt(jnp.mean(wide * wide, -1, keepdims=True) + 1e-6)
    return (wide * scale).astype(BF), wide, scale


def _norm_bwd(wide, scale, d):
    inner = jnp.mean(d * wide, -1, keepdims=True)
    return scale * d - wide * (scale * scale * scale * inner)


def _rows(block, width):
    return pl.BlockSpec((block, width), lambda i: (i, 0))


def _layer_of(w, number):
    return pl.BlockSpec((1, *w.shape[1:]), lambda *_: (number, 0, 0), pipeline_mode=pl.Buffered(1))


def _whole(shape):
    return pl.BlockSpec(shape, lambda *_: (0,) * len(shape))


def _halves(cols):
    half = HEAD // 2
    return [(slice(at, at + half), slice(at + half, at + HEAD)) for at in range(0, cols, HEAD)]


def _qkv(h_ref, cos_ref, sin_ref, wq_ref, wk_ref, wv_ref, q_ref, k_ref, v_ref):
    a, _, _ = _norm(h_ref[...])
    cos, sin = cos_ref[...], sin_ref[...]
    for w_ref, o_ref in ((wq_ref, q_ref), (wk_ref, k_ref)):
        t = _dot(a, w_ref[0], 1, 0).astype(BF).astype(F32)
        for one, two in _halves(t.shape[1]):
            o_ref[:, one] = (t[:, one] * cos - t[:, two] * sin).astype(BF)
            o_ref[:, two] = (t[:, two] * cos + t[:, one] * sin).astype(BF)
    v_ref[...] = _dot(a, wv_ref[0], 1, 0).astype(BF)


def qkv(h, cos, sin, w, number):
    t, d = h.shape
    bt = min(BLOCK, t)
    ws = [w[n] for n in QKV]
    outs = [jax.ShapeDtypeStruct((t, x.shape[2]), BF) for x in ws]
    return pl.pallas_call(
        _qkv,
        grid=(t // bt,),
        in_specs=[_rows(bt, d), _rows(bt, HEAD // 2), _rows(bt, HEAD // 2)] + [_layer_of(x, number) for x in ws],
        out_specs=[_rows(bt, x.shape[1]) for x in outs],
        out_shape=outs,
        compiler_params=_params(1),
        cost_estimate=_cost(2 * t * d * sum(x.shape[2] for x in ws), h, *outs),
        name="qkv",
    )(h, cos, sin, *ws)


def _triangle(n):
    return lax.broadcasted_iota(jnp.int32, (n, n), 1) >= lax.broadcasted_iota(jnp.int32, (n, n), 0)


def _forward(q_ref, k_ref, v_ref, o_ref, lse_ref, top_s, mix_s, *, bq):
    i = pl.program_id(0)
    heads = [(n, slice(n * HEAD, (n + 1) * HEAD)) for n in range(q_ref.shape[1] // HEAD)]
    scale = HEAD**-0.5
    e = scale * LOG2E
    top_s[...] = jnp.full(top_s.shape, NEG, F32)
    mix_s[...] = jnp.zeros_like(mix_s)
    ones = jnp.ones((8, bq), BF)

    def block(j, masked):
        here = pl.ds(pl.multiple_of(j * bq, bq), bq)
        scores = [_dot(k_ref[here, at], q_ref[:, at], 1, 1) for _, at in heads]
        weights, keeps = [], []
        for (n, at), s in zip(heads, scores):
            if masked:
                s = jnp.where(_triangle(bq), s, HIDDEN)
            old = top_s[n : n + 1, :]
            top = jnp.maximum(old, s.max(axis=0, keepdims=True))
            top_s[n : n + 1, :] = top
            weights.append(jnp.exp2((s - top) * e).astype(BF))
            keeps.append(jnp.exp2((old - top) * e))
        for (n, at), p, keep in zip(heads, weights, keeps):
            values = jnp.concatenate([v_ref[here, at].T, ones], axis=0)
            mix_s[n] = mix_s[n] * keep + _dot(values, p, 1, 0)

    lax.fori_loop(0, i, lambda j, _: block(j, False), None)
    block(i, True)
    for n, at in heads:
        total = mix_s[n, HEAD : HEAD + 1, :]
        o_ref[:, at] = (mix_s[n, :HEAD, :] * (1 / total)).T.astype(BF)
        lse_ref[n : n + 1, :] = top_s[n : n + 1, :] * scale + jnp.log(total)


def attend(q, k, v):
    t, cols = q.shape
    bq, n = min(BLOCK, t), cols // HEAD
    return pl.pallas_call(
        functools.partial(_forward, bq=bq),
        grid=(t // bq,),
        in_specs=[_rows(bq, cols), _whole(k.shape), _whole(v.shape)],
        out_specs=[_rows(bq, cols), pl.BlockSpec((n, bq), lambda i: (0, i))],
        out_shape=[jax.ShapeDtypeStruct((t, cols), BF), jax.ShapeDtypeStruct((n, t), F32)],
        scratch_shapes=[pltpu.VMEM((n, bq), F32), pltpu.VMEM((n, HEAD + 8, bq), F32)],
        compiler_params=_params(1),
        cost_estimate=_cost(4 * t * t * cols, q, k, v, q, exps=t * t * n),
        name="attend",
    )(q, k, v)


def _backward(q_ref, k_ref, v_ref, o_ref, do_ref, lse_ref, dq_ref, dk_ref, dv_ref, dq_s, dk_s, dv_s, *, bq):
    i = pl.program_id(0)
    heads = [(n, slice(n * HEAD, (n + 1) * HEAD)) for n in range(q_ref.shape[1] // HEAD)]
    scale = HEAD**-0.5
    e = scale * LOG2E

    @pl.when(i == 0)
    def _():
        dk_s[...] = jnp.zeros_like(dk_s)
        dv_s[...] = jnp.zeros_like(dv_s)

    dq_s[...] = jnp.zeros_like(dq_s)
    lses = [lse_ref[n : n + 1, :] * LOG2E for n, _ in heads]
    deltas = []
    for _, at in heads:
        both = do_ref[:, at].astype(F32) * o_ref[:, at].astype(F32)
        deltas.append((both[:, : HEAD // 2] + both[:, HEAD // 2 :]).T.sum(axis=0, keepdims=True))

    def block(j, masked):
        here = pl.ds(pl.multiple_of(j * bq, bq), bq)
        scores = [_dot(k_ref[here, at], q_ref[:, at], 1, 1) for _, at in heads]
        dps = [_dot(v_ref[here, at], do_ref[:, at], 1, 1) for _, at in heads]
        for n, at in heads:
            p = jnp.exp2(scores[n] * e - lses[n])
            if masked:
                p = jnp.where(_triangle(bq), p, 0.0)
            ds = (p * (dps[n] - deltas[n])).astype(BF)
            dv_s[here, at] += _dot(p.astype(BF), do_ref[:, at], 1, 0)
            dk_s[here, at] += _dot(ds, q_ref[:, at], 1, 0)
            dq_s[n] += _dot(k_ref[here, at].T, ds, 1, 0)

    lax.fori_loop(0, i, lambda j, _: block(j, False), None)
    block(i, True)
    for n, at in heads:
        dq_ref[:, at] = (dq_s[n] * scale).T.astype(BF)

    @pl.when(i == pl.num_programs(0) - 1)
    def _():
        dk_ref[...] = (dk_s[...] * scale).astype(BF)
        dv_ref[...] = dv_s[...].astype(BF)


def attend_bwd(q, k, v, o, do, lse):
    t, cols = q.shape
    bq, n = min(BLOCK, t), cols // HEAD
    out = jax.ShapeDtypeStruct((t, cols), BF)
    return pl.pallas_call(
        functools.partial(_backward, bq=bq),
        grid=(t // bq,),
        in_specs=[_rows(bq, cols), _whole(k.shape), _whole(v.shape), _rows(bq, cols), _rows(bq, cols), pl.BlockSpec((n, bq), lambda i: (0, i))],
        out_specs=[_rows(bq, cols), _whole(k.shape), _whole(v.shape)],
        out_shape=[out] * 3,
        scratch_shapes=[pltpu.VMEM((n, HEAD, bq), F32), pltpu.VMEM((t, cols), F32), pltpu.VMEM((t, cols), F32)],
        compiler_params=_params(1),
        cost_estimate=_cost(6 * t * t * cols, q, k, v, o, do, out, out, out, exps=t * t * n),
        name="attend_bwd",
    )(q, k, v, o, do, lse)


def _ffn(h_ref, o_ref, wo_ref, wg_ref, wu_ref, wd_ref, out_ref, *, piece):
    h2 = h_ref[...] + _dot(o_ref[...], wo_ref[0], 1, 0).astype(BF)
    b, _, _ = _norm(h2)
    total = 0.0
    for at in range(0, wd_ref.shape[1], piece):
        cut = slice(at, at + piece)
        gate, up = _dot(b, wg_ref[0, :, cut], 1, 0), _dot(b, wu_ref[0, :, cut], 1, 0)
        act = (gate * (1 / (1 + jnp.exp(-gate))) * up).astype(BF)
        total = total + _dot(act, wd_ref[0, cut, :], 1, 0)
    out_ref[...] = h2 + total.astype(BF)


def ffn(h, o, w, number):
    t, d = h.shape
    bt = min(BLOCK, t)
    ws = [w[n] for n in ("wo", "w_gate", "w_up", "w_down")]
    ff = w["w_down"].shape[1]
    return pl.pallas_call(
        functools.partial(_ffn, piece=min(512, ff)),
        grid=(t // bt,),
        in_specs=[_rows(bt, d), _rows(bt, o.shape[1])] + [_layer_of(x, number) for x in ws],
        out_specs=_rows(bt, d),
        out_shape=jax.ShapeDtypeStruct((t, d), BF),
        compiler_params=_params(1),
        cost_estimate=_cost(2 * t * d * (o.shape[1] + 3 * ff), h, o, h, exps=t * ff),
        name="ffn",
    )(h, o, *ws)


def _pack(out_ref, at, acc, panels):
    n, width = out_ref.shape[0], out_ref.shape[2]
    rows = acc.shape[0] // n
    for j in range(n):
        for p in range(panels):
            out_ref[j, at + p * rows : at + (p + 1) * rows, :] = acc[j * rows : (j + 1) * rows, p * width : (p + 1) * width].astype(BF)
    return at + panels * rows


def _ffn_bwd(h_ref, o_ref, dy_ref, wo_ref, wg_ref, wu_ref, wd_ref, do_ref, dh_ref, out_ref, g_s, u_s, d_s, o_s, *, piece):
    i = pl.program_id(0)

    @pl.when(i == 0)
    def _():
        for s in (g_s, u_s, d_s, o_s):
            s[...] = jnp.zeros_like(s)

    o, dy = o_ref[...], dy_ref[...]
    h2 = h_ref[...] + _dot(o, wo_ref[0], 1, 0).astype(BF)
    b, wide, scale = _norm(h2)
    by_gate, by_up = 0.0, 0.0
    for at in range(0, wd_ref.shape[1], piece):
        cut = slice(at, at + piece)
        gate, up = _dot(b, wg_ref[0, :, cut], 1, 0), _dot(b, wu_ref[0, :, cut], 1, 0)
        d = _dot(dy, wd_ref[0, cut, :], 1, 1).astype(BF).astype(F32)
        sig = 1 / (1 + jnp.exp(-gate))
        silu = gate * sig
        act = (silu * up).astype(BF)
        d_up = (d * silu).astype(BF)
        d_gate = (d * up * (sig + silu * (1 - sig))).astype(BF)
        d_s[cut, :] += _dot(act, dy, 0, 0)
        g_s[:, cut] += _dot(b, d_gate, 0, 0)
        u_s[:, cut] += _dot(b, d_up, 0, 0)
        by_gate = by_gate + _dot(d_gate, wg_ref[0, :, cut], 1, 1)
        by_up = by_up + _dot(d_up, wu_ref[0, :, cut], 1, 1)
    by_b = (by_gate.astype(BF) + by_up.astype(BF)).astype(F32)
    dh = dy + _norm_bwd(wide, scale, by_b).astype(BF)
    dh_ref[...] = dh
    do_ref[...] = _dot(dh, wo_ref[0], 1, 1).astype(BF)
    o_s[...] += _dot(o, dh, 0, 0)

    @pl.when(i == pl.num_programs(0) - 1)
    def _():
        at = 0
        for s in (g_s, u_s, d_s, o_s):
            at = _pack(out_ref, at, s, s.shape[1] // out_ref.shape[2])


def ffn_bwd(h, o, dy, w, number, n):
    t, d = h.shape
    bt = min(BLOCK, t)
    ws = [w[x] for x in ("wo", "w_gate", "w_up", "w_down")]
    ff, cols = w["w_down"].shape[1], o.shape[1]
    rows = sum(w[x].shape[1] * w[x].shape[2] for x in FFN) // (n * d)
    packed = jax.ShapeDtypeStruct((n, sum(x[0].size for x in w.values()) // (n * d), d), BF)
    return pl.pallas_call(
        functools.partial(_ffn_bwd, piece=min(512, ff)),
        grid=(t // bt,),
        in_specs=[_rows(bt, d), _rows(bt, cols), _rows(bt, d)] + [_layer_of(x, number) for x in ws],
        out_specs=[_rows(bt, cols), _rows(bt, d), pl.BlockSpec((n, rows, d), lambda i: (0, 0, 0), pipeline_mode=pl.Buffered(1))],
        out_shape=[jax.ShapeDtypeStruct((t, cols), BF), jax.ShapeDtypeStruct((t, d), BF), packed],
        scratch_shapes=[pltpu.VMEM((d, ff), F32), pltpu.VMEM((d, ff), F32), pltpu.VMEM((ff, d), F32), pltpu.VMEM((cols, d), F32)],
        compiler_params=_params(1),
        cost_estimate=_cost(2 * t * d * (3 * cols + 8 * ff), h, o, dy, h, o, packed, exps=t * ff),
        name="ffn_bwd",
    )(h, o, dy, *ws)


def _qkv_bwd(h_ref, cos_ref, sin_ref, dq_ref, dk_ref, dv_ref, _, *rest, first, at):
    ins, rest = ([], rest) if first else (rest[:4], rest[4:])
    dh_ref, rest = (None, rest) if first else (rest[0], rest[1:])
    out_ref, pack_s, sem, *sums = rest
    i = pl.program_id(0)

    @pl.when(i == 0)
    def _():
        for s in sums:
            s[...] = jnp.zeros_like(s)

    a, wide, scale = _norm(h_ref[...])
    cos, sin = cos_ref[...], sin_ref[...]
    parts = []
    for d_ref in (dq_ref, dk_ref):
        t = d_ref[...].astype(F32)
        pieces = []
        for one, two in _halves(t.shape[1]):
            pieces += [(t[:, one] * cos + t[:, two] * sin).astype(BF), (t[:, two] * cos - t[:, one] * sin).astype(BF)]
        parts.append(jnp.concatenate(pieces, axis=1))
    parts.append(dv_ref[...])
    for s, p in zip(sums, parts):
        s[...] += _dot(a, p, 0, 0)
    if not first:
        dh2_ref, *ws = ins
        by_a = sum(_dot(p, w[0], 1, 1).astype(BF).astype(F32) for p, w in zip(parts, ws))
        dh_ref[...] = dh2_ref[...] + _norm_bwd(wide, scale, by_a).astype(BF)

    @pl.when(i == pl.num_programs(0) - 1)
    def _():
        to = 0
        for s in sums:
            to = _pack(pack_s, to, s, s.shape[1] // pack_s.shape[2])
        copy = pltpu.make_async_copy(pack_s, out_ref.at[:, at : at + to, :], sem)
        copy.start()
        copy.wait()


def qkv_bwd(h, cos, sin, grads, packed, dh, w, number, n):
    t, d = h.shape
    bt = min(BLOCK, t)
    ws = [w[x] for x in QKV]
    rows = sum(x.shape[1] * x.shape[2] for x in ws) // (n * d)
    first = dh is None
    more = [] if first else [dh, *ws]
    got = pl.pallas_call(
        functools.partial(_qkv_bwd, first=first, at=packed.shape[1] - rows),
        grid=(t // bt,),
        in_specs=[_rows(bt, d), _rows(bt, HEAD // 2), _rows(bt, HEAD // 2)] + [_rows(bt, g.shape[1]) for g in grads] + [pl.BlockSpec(memory_space=pl.ANY)]
        + ([] if first else [_rows(bt, d)] + [_layer_of(x, number) for x in ws]),
        out_specs=([] if first else [_rows(bt, d)]) + [pl.BlockSpec(memory_space=pl.ANY)],
        out_shape=([] if first else [jax.ShapeDtypeStruct((t, d), BF)]) + [jax.ShapeDtypeStruct(packed.shape, BF)],
        input_output_aliases={6: 0 if first else 1},
        scratch_shapes=[pltpu.VMEM((n, rows, d), BF), pltpu.SemaphoreType.DMA] + [pltpu.VMEM(x.shape[1:], F32) for x in ws],
        compiler_params=_params(1),
        cost_estimate=_cost(2 * t * d * (1 if first else 2) * sum(x.shape[2] for x in ws), h, *grads),
        name="qkv_bwd",
    )(h, cos, sin, *grads, packed, *more)
    return (None, got[0]) if first else got


def _factor(*refs, n, count):
    *g_refs, out_ref, part_s, slots, send_sem, recv_sem = refs
    me = lax.axis_index("dp")
    barrier = pltpu.get_barrier_semaphore()
    for k in range(1, n):
        pl.semaphore_signal(barrier, inc=1, device_id={"dp": lax.rem(me + k, n)}, device_id_type=pl.DeviceIdType.MESH)
    total = 0.0
    for g_ref in g_refs:
        g = g_ref[...].astype(F32)
        total = total + (g * g).reshape(g.shape[0] // 8, 8, g.shape[1]).sum(axis=0)
    part = sum(total[:, at : at + 128] for at in range(0, total.shape[1], 128))
    part_s[...] = part
    slots[me] = part
    pl.semaphore_wait(barrier, n - 1)
    copies = [
        pltpu.make_async_remote_copy(
            src_ref=part_s,
            dst_ref=slots.at[me],
            send_sem=send_sem.at[k],
            recv_sem=recv_sem.at[k],
            device_id={"dp": lax.rem(me + k, n)},
            device_id_type=pl.DeviceIdType.MESH,
        )
        for k in range(1, n)
    ]
    for copy in copies:
        copy.start()
    for copy in copies:
        copy.wait()
    squares = jnp.sum(sum(slots[j] for j in range(n)), keepdims=True)
    out_ref[...] = jnp.broadcast_to(jnp.minimum(1.0, 0.5 * lax.rsqrt(squares / count + 1e-30)), out_ref.shape)


def clip_factor(shares, n):
    return pl.pallas_call(
        functools.partial(_factor, n=n, count=n * sum(g.size for g in shares)),
        in_specs=[pl.BlockSpec(memory_space=pltpu.VMEM)] * len(shares),
        out_specs=pl.BlockSpec(memory_space=pltpu.VMEM),
        out_shape=jax.ShapeDtypeStruct((8, 128), F32),
        scratch_shapes=[pltpu.VMEM((8, 128), F32), pltpu.VMEM((n, 8, 128), F32), pltpu.SemaphoreType.DMA((n,)), pltpu.SemaphoreType.DMA((n,))],
        compiler_params=pltpu.CompilerParams(collective_id=0, has_side_effects=True, vmem_limit_bytes=VMEM),
        cost_estimate=_cost(1e6, *shares),
        name="clip_factor",
    )(*shares)


def _adamw(_, factor_ref, *refs, layers, count):
    g_refs, refs = refs[:layers], refs[layers:]
    w_refs, m_refs, v_refs, nm_refs, nv_refs = (dict(zip(NAMES, refs[i * count : (i + 1) * count])) for i in range(5))
    out_ref = refs[5 * count]
    factor = factor_ref[0:1, 0:1]
    width = out_ref.shape[2]
    for number in range(layers):

        @pl.when(pl.program_id(0) == number)
        def _(g_ref=g_refs[number]):
            at = 0
            for name in FFN + QKV:
                rows, cols = w_refs[name].shape[1:]
                for p in range(cols // width):
                    cut = slice(p * width, (p + 1) * width)
                    g = g_ref[at : at + rows, :].astype(F32) * factor
                    m = 0.9 * m_refs[name][0, :, cut] + 0.1 * g
                    v = 0.95 * v_refs[name][0, :, cut] + 0.05 * g * g
                    w = w_refs[name][0, :, cut].astype(F32)
                    nm_refs[name][0, :, cut] = m
                    nv_refs[name][0, :, cut] = v
                    out_ref[0, at : at + rows, :] = (w - 0.02 * (m * lax.rsqrt(v + 1e-8) + 0.1 * w)).astype(BF)
                    at += rows


def adamw(me, factor, shares, weights, m, v):
    layers, d = weights[0].shape[0], shares[0].shape[1]
    rows = sum(x.shape[0] for x in shares) // layers
    own = [pl.BlockSpec((1, *one.shape[1:]), lambda i, me: (i, me[0], 0)) for one in m]
    here = [pl.BlockSpec((1, *one.shape[1:]), lambda i, me: (i, 0, 0)) for one in m]
    got = pl.pallas_call(
        functools.partial(_adamw, layers=layers, count=len(m)),
        grid_spec=pltpu.PrefetchScalarGridSpec(
            num_scalar_prefetch=1,
            grid=(layers,),
            in_specs=[pl.BlockSpec(x.shape, lambda i, me: (0, 0)) for x in (factor, *shares)] + own + here + here,
            out_specs=here + here + [pl.BlockSpec((1, rows, d), lambda i, me: (i, 0, 0))],
        ),
        out_shape=[jax.ShapeDtypeStruct(x.shape, F32) for x in (*m, *m)] + [jax.ShapeDtypeStruct((layers, rows, d), BF)],
        compiler_params=_params(1),
        cost_estimate=_cost(20 * layers * rows * d, *m, *m, *m, *m),
        name="adamw",
    )(me[None], factor, *shares, *weights, *m, *v)
    k = len(m)
    return got[:k], got[k : 2 * k], got[2 * k]


def _unpack(in_ref, *out_refs):
    outs = dict(zip(NAMES, out_refs))
    width = in_ref.shape[3]
    for number in range(in_ref.shape[1]):
        at = 0
        for name in FFN + QKV:
            rows, cols = outs[name].shape[1:]
            for p in range(cols // width):
                outs[name][number, :, p * width : (p + 1) * width] = in_ref[0, number, at : at + rows, :]
                at += rows


def unpack(packed, shapes):
    n = packed.shape[0]
    return pl.pallas_call(
        _unpack,
        grid=(n,),
        in_specs=[pl.BlockSpec((1, *packed.shape[1:]), lambda j: (j, 0, 0, 0))],
        out_specs=[pl.BlockSpec((s[0], s[1] // n, s[2]), lambda j: (0, j, 0)) for s in shapes],
        out_shape=[jax.ShapeDtypeStruct(s, BF) for s in shapes],
        compiler_params=_params(1),
        cost_estimate=_cost(0, packed, packed),
        name="unpack",
    )(packed)


def solution(mesh):
    n = mesh.shape["dp"]

    def step(x, dy, *arrays):
        weights, m, v = (arrays[i : i + 7] for i in (0, 7, 14))
        w = dict(zip(NAMES, weights, strict=True))
        layers = weights[0].shape[0]
        half = HEAD // 2
        angle = jnp.arange(x.shape[1], dtype=F32)[:, None] * THETA ** (-jnp.arange(half, dtype=F32) / half)
        cos, sin = jnp.cos(angle), jnp.sin(angle)
        h, kept = x[0], []
        for number in range(layers):
            q, k, val = qkv(h, cos, sin, w, number)
            o, lse = attend(q, k, val)
            kept.append((h, q, k, val, o, lse))
            if number < layers - 1:
                h = ffn(h, o, w, number)
        d, shares = dy[0], [None] * layers
        scatter = lambda g: lax.psum_scatter(g, "dp", scatter_dimension=0, tiled=False)
        for number in reversed(range(layers)):
            h, q, k, val, o, lse = kept[number]
            do, dh, packed = ffn_bwd(h, o, d, w, number, n)
            grads = attend_bwd(q, k, val, o, do, lse)
            d, packed = qkv_bwd(h, cos, sin, grads, packed, dh if number else None, w, number, n)
            shares[number] = scatter(packed)
        factor = clip_factor(shares, n)
        new_m, new_v, packed = adamw(lax.axis_index("dp"), factor, shares, weights, m, v)
        new_w = unpack(lax.all_gather(packed, "dp", axis=0, tiled=False), [one.shape for one in weights])
        return (*new_w, *new_m, *new_v)

    states, all_of, cut = P(("rep", "dp"), None, None), P(None, None, None), P(None, "dp", None)
    return jax.shard_map(
        step,
        mesh=mesh,
        in_specs=(states, states) + (all_of,) * 7 + (cut,) * 14,
        out_specs=(P("rep", None, None),) * 7 + (P("rep", "dp", None),) * 14,
        check_vma=False,
    )
```
